32 devices in a mesh: seq: 4 (over z), exp: 8 (over y, x, core).
Axes of the slice: x: 2, y: 2, z: 4, core: 2. Of those that a mesh axis runs over, the one named last changes fastest.
Arguments:
- tokens: bfloat16 [20480, 4096], P(('seq', 'exp')), may hold values from -6 to 6
- routes: int32 [20480, 2], P(('seq', 'exp')), may hold values from 0 to 15, all different within a row; in each aligned block of 640 rows (0 to 639, 640 to 1279, ...) at most 100 rows name the same one
- gates: float32 [20480, 2], P(('seq', 'exp')), may hold values from 0.1 to 1
- weights: bfloat16 [16, 4096, 1024], P('exp', 'seq'), may hold values from -0.09375 to 0.09375
Outputs:
- mixed: bfloat16 [20480, 1024], P(('seq', 'exp'))
The draws below stay inside these ranges and needn't reach their ends.
Inputs may be any that keep to these rules, and one draw needn't show every extreme that they name: `routes`: the two experts of a token differ. Among the rows of one device no expert is named more than 100 times, a bound that some block reaches.
All inputs are finite; a program needn't handle non-finite values.
Results may differ from the reference program's by a relative error of at most 0.0049.
Values may be sent and summed in bfloat16 or wider, within the bound.
A program may use at most 192 MiB of HBM per device.

```python
import math
import jax
import jax.numpy as jnp
import numpy as np
from jax import lax

D = 4096
FF = 1024
TOK_DEV = 640
EXPERTS = 16
CAP = 100
TOKENS = 20480


def levels(rng, shape, shards, low, high):
    factor_of = 1.0
    for dim, shards_of in shards:
        draws = jax.random.uniform(jax.random.fold_in(jax.random.fold_in(rng, 6), dim), (shards_of,), jnp.float32, low / len(shards), high / len(shards))
        factor_of = factor_of * jnp.repeat(jnp.exp(draws), shape[dim] // shards_of).reshape((-1,) + (1,) * (len(shape) - 1 - dim))
    return factor_of


def deal_out(stream_key, own, number, rows, amount, top, limit, slope):
    sequence = jax.random.permutation(stream_key, amount)
    crowded, common = shares(amount, rows * top, limit, slope, True), shares(amount, rows * top, limit, slope, False)
    places = jnp.arange(amount)

    def named(lengths, turn):
        used = int((lengths > 0).sum())
        fixed = max(1, used // 4)
        shifted = fixed + (places - fixed + turn * (used - fixed)) % max(1, amount - fixed)
        return jnp.zeros((amount,), jnp.int32).at[sequence[jnp.where(places < fixed, places, shifted)]].set(jnp.asarray(lengths, jnp.int32))

    lengths = jnp.where(number % 4 == 0, named(crowded, number // 4), named(common, number - number // 4 - 1))
    mixed = jax.random.permutation(jax.random.fold_in(own, 3), amount)
    donor, sink = mixed[0:amount // 2 * 2:2], mixed[1:amount // 2 * 2:2]
    margin = jnp.minimum(lengths[donor] - 1, limit - lengths[sink]) // 2
    margin = jnp.where((donor == sequence[0]) | (sink == sequence[0]) | (lengths[sink] == 0), 0, jnp.maximum(margin, 0))
    shifted = jax.random.randint(jax.random.fold_in(own, 4), (amount // 2,), 0, 1 << 20) % (margin + 1)
    lengths = lengths.at[donor].add(-shifted).at[sink].add(shifted)
    items = jnp.searchsorted(jnp.cumsum(lengths), jnp.arange(rows * top), side="right").astype(jnp.int32)
    grid = items.reshape(top, rows).T
    grid = grid[jax.random.permutation(jax.random.fold_in(own, 1), rows)]
    turn = jax.random.randint(jax.random.fold_in(own, 2), (rows, 1), 0, top)
    return jnp.take_along_axis(grid, (jnp.arange(top)[None, :] + turn) % top, axis=1)


def shares(number_of, total, most, skew, full):
    weights = [(1 << 20) // math.isqrt(standing ** skew) + 1 for standing in range(1, number_of + 1)]
    largest = most if full else min(most, max(-(-total // number_of), total * weights[0] // sum(weights)))
    least = 1 if total - largest >= number_of - 1 else 0
    holding, rest = [largest] + [least] * (number_of - 1), total - largest - least * (number_of - 1)
    while rest > 0:
        free = [i for i in range(1, number_of) if holding[i] < largest] or [i for i in range(1, number_of) if holding[i] < most]
        mass, budget = sum([weights[i] for i in free]), rest
        for i in free:
            more = min(most - holding[i], max(1, budget * weights[i] // mass), rest)
            holding[i] = holding[i] + more
            rest = rest - more
    return np.array(holding)


def scatter_about(rng, extent, scale, most, pieces=(), held_as=jnp.bfloat16):
    gain = levels(rng, extent, pieces, -0.22, 0.18) if pieces else 1.0
    drawn = jax.random.normal(rng, extent, jnp.float32) * scale * gain
    return jnp.minimum(jnp.maximum(drawn, -most), most).astype(held_as)


def setup_inputs(seed: int = 0) -> dict:
    seeds = jax.random.split(jax.random.key(seed), 5)
    tokens = scatter_about(seeds[0], (TOKENS, D), 1.0, 6.0, ((0, 32),))
    routes_keys = jax.random.split(jax.random.fold_in(seeds[1], 1), TOKENS // TOK_DEV)
    routes_turns = jax.random.permutation(jax.random.fold_in(seeds[1], 3), TOKENS // TOK_DEV)
    routes = jax.vmap(lambda own, number: deal_out(jax.random.fold_in(seeds[1], 2), own, number, TOK_DEV, EXPERTS, 2, CAP, 2))(routes_keys, routes_turns).reshape((TOKENS, 2))
    gates = jnp.clip(0.1 + 0.9 * jax.random.uniform(seeds[2], (TOKENS, 2), jnp.float32) ** levels(seeds[2], (TOKENS, 2), ((0, 32),), -0.2, 0.2), 0.1, 1.0)
    weights = scatter_about(seeds[3], (EXPERTS, D, FF), D ** -0.5, 0.09375, ((0, 8), (1, 4)))
    return dict(tokens=tokens, routes=routes, gates=gates, weights=weights)


def route_slots(route_block, experts, capacity):
    expert_ids = route_block.reshape(-1)
    one_hot = (expert_ids[:, None] == jnp.arange(experts, dtype=jnp.int32)[None, :]).astype(jnp.int32)
    earlier = jnp.cumsum(one_hot, axis=0) - one_hot
    slot_index = jnp.sum(earlier * one_hot, axis=1)
    return (expert_ids * capacity + slot_index).astype(jnp.int32)


def reference(tokens, routes, gates, weights):
    blocks = TOKENS // TOK_DEV
    route_blocks = routes.reshape(blocks, TOK_DEV, 2)
    position = jax.vmap(lambda block: route_slots(block, EXPERTS, CAP))(route_blocks)
    local_rows = jnp.arange(2 * TOK_DEV, dtype=jnp.int32) // 2
    block_base = (jnp.arange(blocks, dtype=jnp.int32) * TOK_DEV)[:, None]
    global_rows = block_base + local_rows[None, :]

    def fill_table(places, rows):
        return jnp.full((EXPERTS * CAP,), TOKENS, jnp.int32).at[places].set(rows)

    slot_rows = jax.vmap(fill_table)(position, global_rows).reshape(blocks, EXPERTS, CAP)
    padded = jnp.concatenate([tokens, jnp.zeros((1, D), jnp.bfloat16)], axis=0)

    def one_expert(expert):
        indices = lax.dynamic_index_in_dim(slot_rows, expert, 1, keepdims=False).reshape(-1)
        gathered = padded[indices]
        matrix = lax.dynamic_index_in_dim(weights, expert, 0, keepdims=False)
        return jnp.dot(gathered, matrix, preferred_element_type=jnp.float32).astype(jnp.bfloat16)

    outputs = lax.map(one_expert, jnp.arange(EXPERTS, dtype=jnp.int32))
    outputs = outputs.reshape(EXPERTS * blocks * CAP, FF)
    expert_ids = route_blocks.reshape(blocks, 2 * TOK_DEV)
    slot_index = position - expert_ids * CAP
    block_ids = jnp.arange(blocks, dtype=jnp.int32)[:, None]
    flat_index = ((expert_ids * blocks + block_ids) * CAP + slot_index).reshape(-1)
    picked = outputs[flat_index].reshape(TOKENS, 2, FF).astype(jnp.float32)
    mixed = jnp.sum(picked * gates[:, :, None], axis=1)
    return mixed.astype(jnp.bfloat16)
```

```python
import functools

import jax
import jax.numpy as jnp
from jax import lax
from jax.experimental import pallas as pl
from jax.experimental.pallas import tpu as pltpu
from jax.sharding import PartitionSpec as P

COLUMN_PARTS = (1, 1)


def project_kernel(per_step, x_ref, gate_ref, w_ref, *rest):
    out_ref = rest[-1]
    step = pl.program_id(0)
    lanes = lax.broadcasted_iota(jnp.int32, gate_ref.shape, 1)

    @pl.when(step == 0)
    def _():
        out_ref[...] = jnp.zeros_like(out_ref)

    total = out_ref[...]
    for own in range(per_step):
        expert = step * per_step + own
        gate = jnp.sum(jnp.where(lanes == expert, gate_ref[...], 0.0), axis=1, keepdims=True)
        total += gate * jnp.dot(x_ref[...], w_ref[own], preferred_element_type=jnp.float32)
    out_ref[...] = total


def project(x, gate, weights, before):
    rows, depth = x.shape
    experts, _, cols = weights.shape
    per_step = 2
    return pl.pallas_call(
        functools.partial(project_kernel, per_step),
        grid=(experts // per_step,),
        out_shape=jax.ShapeDtypeStruct((rows, cols), jnp.float32),
        in_specs=[
            pl.BlockSpec((rows, depth), lambda e: (0, 0)),
            pl.BlockSpec((rows, experts), lambda e: (0, 0)),
            pl.BlockSpec((per_step, depth, cols), lambda e: (e, 0, 0)),
        ]
        + [pl.BlockSpec(memory_space=pl.ANY)] * len(before),
        out_specs=pl.BlockSpec((rows, cols), lambda e: (0, 0)),
        compiler_params=pltpu.CompilerParams(vmem_limit_bytes=32 * 1024 * 1024),
        cost_estimate=pl.CostEstimate(
            flops=2 * rows * depth * cols * experts,
            bytes_accessed=2 * experts * depth * cols + 2 * rows * depth,
            transcendentals=0,
        ),
    )(x, gate, weights, *before)


def shift_order(planes):
    near = [d for pair in zip(range(1, planes), range(planes - 1, 0, -1)) for d in pair]
    return list(dict.fromkeys(near))


def unit_order(planes, parts):
    early = 1
    arrival = [0] + shift_order(planes)
    order = [(d, q) for q in range(early) for d in arrival[:-1]]
    order += [(arrival[-1], q) for q in range(early)]
    for q in range(early, parts):
        order += [(d, q) for d in list(range(1, planes)) + [0]]
    return order


def body(tokens, routes, gates, weights):
    experts = weights.shape[0] * lax.axis_size("exp")
    planes = lax.axis_size("seq")
    plane = lax.axis_index("seq")
    depth = weights.shape[1]
    share = weights.shape[2] // sum(COLUMN_PARTS)
    edges = [share * sum(COLUMN_PARTS[:q]) for q in range(len(COLUMN_PARTS) + 1)]

    def moved(value, shift):
        return lax.ppermute(value, "seq", [(i, (i + shift) % planes) for i in range(planes)])

    def features(target):
        return lax.dynamic_slice_in_dim(tokens, target * depth, depth, 1)

    dense = jnp.sum(
        jnp.where(
            routes[:, None, :] == jnp.arange(experts, dtype=jnp.int32)[None, :, None],
            gates[:, None, :],
            0.0,
        ),
        axis=2,
    )
    sent = dense.T
    gate, x = {0: dense}, {0: features(plane)}
    for shift in range(1, planes):
        gate[shift] = moved(sent, shift).T
    latest = None
    for shift in shift_order(planes):
        piece = features(lax.rem(plane + shift, planes))
        if latest is not None:
            piece, _ = lax.optimization_barrier((piece, latest))
        latest = x[shift] = moved(piece, shift)
    whole = [
        lax.all_gather(weights[:, :, edges[q] : edges[q + 1]], "exp", axis=0, tiled=True)
        for q in range(len(COLUMN_PARTS))
    ]
    parts, running, flying, stage, started = {}, {}, {}, {}, {}
    previous = []
    for index, (shift, q) in enumerate(unit_order(planes, len(COLUMN_PARTS))):
        landed = [key for key in flying if started[key] <= index - 2 and index >= planes]
        done = project(x[shift], gate[shift], whole[q], previous + [flying.pop(key) for key in landed])
        previous = [done]
        parts[shift, q] = done
        at = stage.get(q, 1)
        while at <= planes and (at % planes, q) in parts:
            begin = index
            value = parts[at % planes, q]
            if at > 1:
                value = running[q].astype(jnp.float32) + value
                begin = max(begin, started[at - 1, q] + 1)
            running[q] = value.astype(jnp.bfloat16)
            if at < planes:
                running[q] = moved(running[q], 1)
                flying[at, q] = running[q]
                started[at, q] = begin
            at += 1
        stage[q] = at
    return jnp.concatenate([running[q] for q in range(len(COLUMN_PARTS))], axis=1)


def solution(mesh):
    return jax.shard_map(
        body,
        mesh=mesh,
        in_specs=(
            P(("seq", "exp"), None),
            P(("seq", "exp"), None),
            P(("seq", "exp"), None),
            P("exp", "seq", None),
        ),
        out_specs=P(("seq", "exp"), None),
        check_vma=False,
    )
```
